32 devices in a mesh: rep: 2 (over core), seq: 16 (over z, y, x).
Axes of the slice: x: 2, y: 2, z: 4, core: 2. Of those that a mesh axis runs over, the one named last changes fastest.
Arguments:
- queries: bfloat16 [4096, 8192], P(('rep', 'seq')), parts along dimension 0, may hold values from -180 to 180
- keys: bfloat16 [16384, 1024], P(('rep', 'seq')), parts along dimension 0, may hold values from -6 to 6
- values: bfloat16 [16384, 1024], P(('rep', 'seq')), parts along dimension 0, may hold values from -6 to 6
- vertical: int32 [128, 64], P('rep'), parts along dimension 0, may hold values from 0 to 127, all different within a row
- vert_count: int32 [128], P('rep'), parts along dimension 0, may hold values from 1 to 64
- slash: int32 [128, 32], P('rep'), parts along dimension 0, may hold values from 0 to 95, all different within a row
- slash_count: int32 [128], P('rep'), parts along dimension 0, may hold values from 1 to 32
Outputs:
- attended: bfloat16 [4096, 8192], P(('rep', 'seq')), parts along dimension 0
The draws below stay inside these ranges and needn't reach their ends.
There are 2 independent parts, one for each index of `rep`. The reference program is written for one: setup_inputs(seed, part) draws one part's arguments, and reference() takes and returns one part's arrays. A program takes and returns all parts, laid end to end along the dimension named above; each array names one. Nothing has to cross between parts.
Inputs may be any that keep to these rules, and one draw needn't show every extreme that they name: `vertical`: each row holds 64 different key block numbers; head h uses the first vert_count[h] of them. `slash`: each row holds 32 different numbers; head h uses the first slash_count[h] of them, each number s naming the slash offset s + 1 blocks.
All inputs are finite; a program needn't handle non-finite values.
Results may differ from the reference program's by a relative error of at most 0.007.
Values may be sent and summed in bfloat16 or wider, within the bound.
No kernel may reach another device: no remote copies, remote signals or barrier semaphores. Data moves between devices by JAX's collectives and lax.ppermute only.
A program may use at most 128 MiB of HBM per device.

```python
import math
import jax
import jax.numpy as jnp
from jax import lax

QUERY_HEADS = 64
KV_HEADS = 8
HEAD_DIM = 128
BLOCK = 64
VERT = 64
SLASHES = 32
QUERIES = 2048
CONTEXT = 8192
QBLOCKS = 32
KBLOCKS = 128
SPAN = 96


def make_pair(key):
    base_keys = jnp.clip(jax.random.normal(jax.random.fold_in(key, 101), (CONTEXT, KV_HEADS, HEAD_DIM), jnp.float32), -6.0, 6.0)
    base_queries = jnp.clip(jax.random.normal(jax.random.fold_in(key, 102), (QUERIES, QUERY_HEADS, HEAD_DIM), jnp.float32), -6.0, 6.0)
    return (base_queries.reshape(QUERIES, QUERY_HEADS * HEAD_DIM), base_keys.reshape(CONTEXT, KV_HEADS * HEAD_DIM))


def draw_queries(key, part):
    return make_pair(key)[0].astype(jnp.bfloat16)


def draw_keys(key, part):
    return make_pair(key)[1].astype(jnp.bfloat16)


def set_ends(entries, stream_key, smallest, high):
    index_at = [jax.random.randint(jax.random.fold_in(stream_key, axis), (), 0, length) for axis, length in enumerate(entries.shape)]
    longest = entries.shape.index(max(entries.shape))
    neighbour = index_at[:longest] + [(index_at[longest] + 1) % entries.shape[longest]] + index_at[longest + 1:]
    return entries.at[tuple(index_at)].set(smallest).at[tuple(neighbour)].set(high)


def block_levels(rng, extent, split, smallest, top_value):
    loudness = 1.0
    for axis_at, blocks in split:
        heights = jax.random.uniform(jax.random.fold_in(jax.random.fold_in(rng, 6), axis_at), (blocks,), jnp.float32, smallest / len(split), top_value / len(split))
        loudness = loudness * jnp.repeat(jnp.exp(heights), extent[axis_at] // blocks).reshape((-1,) + (1,) * (len(extent) - 1 - axis_at))
    return loudness


def distinct(own_key, rows, count, top, lift):
    order = jax.random.permutation(jax.random.fold_in(own_key, 1), count)
    favour = order
    for power in range(3):
        favour = favour * favour // count
    favour = favour * lift // count
    chance = jax.random.randint(jax.random.fold_in(own_key, 2), (rows, count), 0, 4096) + favour
    holders = jax.random.permutation(jax.random.fold_in(own_key, 3), rows)[jnp.arange(count) % rows]
    chance = jnp.where(jnp.arange(rows)[:, None] == holders[None, :], 1 << 14, chance)
    score = chance * count + jnp.arange(count)
    return lax.top_k(score.astype(jnp.int32), top)[1].astype(jnp.int32)


def scatter_about(rng, extent, scale, bound, split=(), kind=jnp.bfloat16):
    values = jax.random.normal(rng, extent, jnp.float32) * scale
    if len(split) > 0:
        values = block_levels(rng, extent, split, -0.22, 0.18) * values
    return jnp.clip(values, min=-bound, max=bound).astype(kind)


def setup_inputs(seed: int = 0, part: int = 0) -> dict:
    seeds = jax.random.split(jax.random.key(seed), 8)
    part_splits = jax.random.split(jax.random.fold_in(seeds[7], part), 8)
    queries = draw_queries(jax.random.fold_in(jax.random.fold_in(seeds[7], part), 71), part)
    keys = draw_keys(jax.random.fold_in(jax.random.fold_in(seeds[7], part), 71), part)
    values = scatter_about(part_splits[2], (CONTEXT, KV_HEADS * HEAD_DIM), 1.0, 6.0, ((0, 16),))
    vertical = distinct(part_splits[3], QUERY_HEADS, KBLOCKS, VERT, 0)
    vert_count = set_ends(jax.random.randint(part_splits[4], (QUERY_HEADS,), 1, VERT + 1), jax.random.fold_in(part_splits[4], 1), 1, VERT).astype(jnp.int32)
    slash = distinct(part_splits[5], QUERY_HEADS, SPAN, SLASHES, 0)
    slash_count = set_ends(jax.random.randint(part_splits[6], (QUERY_HEADS,), 1, SLASHES + 1), jax.random.fold_in(part_splits[6], 1), 1, SLASHES).astype(jnp.int32)
    return {"queries": queries, "keys": keys, "values": values, "vertical": vertical, "vert_count": vert_count, "slash": slash, "slash_count": slash_count}


def reference(queries, keys, values, vertical, vert_count, slash, slash_count):
    per_group = QUERY_HEADS // KV_HEADS
    query_grid = queries.reshape(QBLOCKS, BLOCK, QUERY_HEADS, HEAD_DIM)
    key_grid = keys.reshape(KBLOCKS, BLOCK, KV_HEADS, HEAD_DIM)
    value_grid = values.reshape(KBLOCKS, BLOCK, KV_HEADS, HEAD_DIM)
    absolute = (KBLOCKS - QBLOCKS + jnp.arange(QBLOCKS, dtype=jnp.int32)).astype(jnp.int32)
    scale = 1.0 / math.sqrt(HEAD_DIM)
    causal = jnp.arange(BLOCK)[:, None] >= jnp.arange(BLOCK)[None, :]
    exact = lax.Precision.HIGHEST

    def one_head(head):
        group = head // per_group
        query = jnp.take(query_grid, head, axis=2).astype(jnp.float32)
        key_set = jnp.take(key_grid, group, axis=2)
        value_set = jnp.take(value_grid, group, axis=2)
        verticals = vertical[head]
        live_vert = vert_count[head]
        offsets = (slash[head] + 1).astype(jnp.int32)
        live_slash = slash_count[head]
        marks = jnp.arange(VERT, dtype=jnp.int32) < live_vert
        target = (absolute[:, None] - offsets[None, :]).astype(jnp.int32)
        own_keys = key_set[absolute].astype(jnp.float32)
        own_values = value_set[absolute].astype(jnp.float32)
        vert_keys = key_set[verticals].reshape(VERT * BLOCK, HEAD_DIM).astype(jnp.float32)
        vert_values = value_set[verticals].reshape(VERT * BLOCK, HEAD_DIM).astype(jnp.float32)
        slash_keys = key_set[target].reshape(QBLOCKS, SLASHES * BLOCK, HEAD_DIM).astype(jnp.float32)
        slash_values = value_set[target].reshape(QBLOCKS, SLASHES * BLOCK, HEAD_DIM).astype(jnp.float32)
        own_scores = jnp.einsum('rqd,rkd->rqk', query, own_keys, precision=exact) * scale
        vert_scores = jnp.einsum('rqd,kd->rqk', query, vert_keys, precision=exact) * scale
        slash_scores = jnp.einsum('rqd,rkd->rqk', query, slash_keys, precision=exact) * scale
        vert_ok = marks[None, :] & (verticals[None, :] < absolute[:, None])
        covered = jnp.any((target[:, :, None] == verticals[None, None, :]) & marks[None, None, :], axis=2)
        slash_ok = (jnp.arange(SLASHES, dtype=jnp.int32) < live_slash)[None, :] & jnp.logical_not(covered)
        own_valid = jnp.broadcast_to(causal[None], (QBLOCKS, BLOCK, BLOCK))
        vert_valid = jnp.broadcast_to(jnp.repeat(vert_ok, BLOCK, axis=1)[:, None, :], (QBLOCKS, BLOCK, VERT * BLOCK))
        slash_valid = jnp.broadcast_to(jnp.repeat(slash_ok, BLOCK, axis=1)[:, None, :], (QBLOCKS, BLOCK, SLASHES * BLOCK))
        scores = jnp.concatenate([own_scores, vert_scores, slash_scores], axis=2)
        valid = jnp.concatenate([own_valid, vert_valid, slash_valid], axis=2)
        scores = jnp.where(valid, scores, -jnp.inf)
        peak = lax.optimization_barrier(jnp.max(scores, axis=2, keepdims=True))
        weights = jnp.exp(scores - peak)
        total = lax.optimization_barrier(jnp.sum(weights, axis=2, keepdims=True))
        rounded = lax.optimization_barrier(weights.astype(jnp.bfloat16)).astype(jnp.float32)
        first_cut = BLOCK
        second_cut = BLOCK + VERT * BLOCK
        result = jnp.einsum('rqk,rkd->rqd', rounded[:, :, :first_cut], own_values, precision=exact)
        result = result + jnp.einsum('rqk,kd->rqd', rounded[:, :, first_cut:second_cut], vert_values, precision=exact)
        result = result + jnp.einsum('rqk,rkd->rqd', rounded[:, :, second_cut:], slash_values, precision=exact)
        return (result / total).astype(jnp.bfloat16)
    heads = lax.map(one_head, jnp.arange(QUERY_HEADS, dtype=jnp.int32))
    return heads.transpose(1, 2, 0, 3).reshape(QUERIES, QUERY_HEADS * HEAD_DIM)
```

```python
import math
import functools
import jax, jax.numpy as jnp
from jax import lax
from jax.experimental import pallas as pl
from jax.experimental.pallas import tpu as pltpu
from jax.sharding import PartitionSpec as P

BLOCK=64
HEAD_DIM=128
LANES=128
ONES=16
HIDE=-1e30

def attention_kernel(factor, pieces, side_ref, table_ref, q_ref, *refs):
    kv_refs, (out_ref, kfull, vt, qa, stage, sa, sb, acc) = refs[:pieces], refs[pieces:]
    head, tile = pl.program_id(0), pl.program_id(1)
    tiles = pl.num_programs(1)
    senders, piece_rows, _ = kv_refs[0].shape
    chunk = pieces * piece_rows
    width = HEAD_DIM
    rows = q_ref.shape[0]

    @pl.when((head == 0) & (tile == 0))
    def _():
        vt[width:, :] = jnp.ones((ONES, vt.shape[1]), vt.dtype)

        def fill(sender, carry):
            at = pl.multiple_of(sender * chunk, chunk)
            for p in range(pieces):
                piece = p ^ side_ref[0]
                spot = pl.multiple_of(at + piece * piece_rows, piece_rows)
                kfull[pl.ds(spot, piece_rows), :width] = kv_refs[p][sender][:, :width]
                stage[pl.ds(pl.multiple_of(piece * piece_rows, piece_rows), piece_rows), :] = kv_refs[p][sender][:, width:]
            vt[:width, pl.ds(at, chunk)] = stage[...].T
            return carry

        lax.fori_loop(0, senders, fill, 0)

    @pl.when(tile == 0)
    def _():
        def fill(group, carry):
            for u in range(8):
                block = group * 8 + u
                row = table_ref[0, pl.ds(block, 1), :]
                at = pl.multiple_of(block * BLOCK, BLOCK)
                kfull[pl.ds(at, BLOCK), width:] = jnp.broadcast_to(row, (BLOCK, row.shape[1])).astype(jnp.bfloat16)
            return carry

        lax.fori_loop(0, table_ref.shape[1] // 8, fill, 0)

    qa[:width, :] = q_ref[...].T
    lane_block = lax.broadcasted_iota(jnp.int32, (qa.shape[0] - width, rows), 1) // BLOCK + tile * (rows // BLOCK)
    qa[width:, :] = (lax.broadcasted_iota(jnp.int32, (qa.shape[0] - width, rows), 0) == lane_block).astype(jnp.float32).astype(jnp.bfloat16)
    acc[...] = jnp.zeros_like(acc)
    own = senders - tiles + tile
    count = own + 1

    def where_at(step):
        return pl.multiple_of(jnp.where(step == 0, own, jnp.minimum(step - 1, own)) * chunk, chunk)

    def score(step, s_ref):
        s = jnp.dot(kfull[pl.ds(where_at(step), chunk), :], qa[...], preferred_element_type=jnp.float32)
        s_ref[...] = s
        return jnp.max(s.reshape(chunk // 8, 8, rows), axis=0)

    def fold(step, s_ref, peak, part):
        top = jnp.maximum(peak, jnp.max(part, axis=0, keepdims=True))
        alpha = jnp.exp2((peak - top) * factor)
        p = jnp.exp2((s_ref[...] - top) * factor).astype(jnp.bfloat16)
        acc[...] = acc[...] * alpha + jnp.dot(vt[:, pl.ds(where_at(step), chunk)], p, preferred_element_type=jnp.float32)
        return top

    s = jnp.dot(kfull[pl.ds(where_at(0), chunk), :], qa[...], preferred_element_type=jnp.float32)
    s = jnp.where(lax.broadcasted_iota(jnp.int32, s.shape, 0) <= lax.broadcasted_iota(jnp.int32, s.shape, 1), s, HIDE)
    sa[...] = s
    part = jnp.max(s.reshape(chunk // 8, 8, rows), axis=0)
    peak = jnp.full((1, rows), HIDE, jnp.float32)

    def pair(i, carry):
        peak, part = carry
        part_b = score(2 * i + 1, sb)
        peak = fold(2 * i, sa, peak, part)
        part = score(2 * i + 2, sa)
        peak = fold(2 * i + 1, sb, peak, part_b)
        return peak, part

    peak, part = lax.fori_loop(0, count // 2, pair, (peak, part))

    @pl.when(count % 2 == 1)
    def _():
        fold(count - 1, sa, peak, part)

    total = acc[width:width + 1, :]
    out_ref[...] = (acc[:width, :] / total).T.astype(out_ref.dtype)


def attention(q, cache, table, side):
    pieces = len(cache)
    senders, piece_rows, _ = cache[0].shape
    chunk = pieces * piece_rows
    heads = q.shape[1] // HEAD_DIM
    tiles = q.shape[0] // chunk
    context = senders * chunk
    lanes = table.shape[2]
    factor = math.log2(math.e) / math.sqrt(HEAD_DIM)
    pairs = heads * q.shape[0] * context
    return pl.pallas_call(
        functools.partial(attention_kernel, factor, pieces),
        out_shape=jax.ShapeDtypeStruct(q.shape, jnp.bfloat16),
        grid_spec=pltpu.PrefetchScalarGridSpec(
            num_scalar_prefetch=1,
            grid=(heads, tiles),
            in_specs=[
                pl.BlockSpec((1, table.shape[1], lanes), lambda h, t, s: (h, 0, 0)),
                pl.BlockSpec((chunk, HEAD_DIM), lambda h, t, s: (t, h)),
            ]
            + [pl.BlockSpec(x.shape, lambda h, t, s: (0, 0, 0), pipeline_mode=pl.Buffered(1)) for x in cache],
            out_specs=pl.BlockSpec((chunk, HEAD_DIM), lambda h, t, s: (t, h)),
            scratch_shapes=[
                pltpu.VMEM((context, HEAD_DIM + lanes), jnp.bfloat16),
                pltpu.VMEM((HEAD_DIM + ONES, context), jnp.bfloat16),
                pltpu.VMEM((HEAD_DIM + lanes, chunk), jnp.bfloat16),
                pltpu.VMEM((chunk, HEAD_DIM), jnp.bfloat16),
                pltpu.VMEM((chunk, chunk), jnp.float32),
                pltpu.VMEM((chunk, chunk), jnp.float32),
                pltpu.VMEM((HEAD_DIM + ONES, chunk), jnp.float32),
            ],
        ),
        compiler_params=pltpu.CompilerParams(
            dimension_semantics=("arbitrary", "arbitrary"), vmem_limit_bytes=67000000
        ),
        cost_estimate=pl.CostEstimate(
            flops=4 * pairs * HEAD_DIM,
            bytes_accessed=4 * q.size + 2 * pieces * cache[0].size,
            transcendentals=pairs,
        ),
        name="attention",
    )(side, table, q, *cache)


QUERY_HEADS = 64
KV_HEADS = 8
GROUPS = 4


def swapped(x, axis, bit):
    return lax.ppermute(x, axis, [(i, i ^ 1 << bit) for i in range(lax.axis_size(axis))])


def mask_table(first, heads, blocks, stretch, vertical, vert_count, slash, slash_count):
    lanes = -(-stretch // LANES) * LANES
    take = lambda x: lax.dynamic_slice_in_dim(x, first, heads, 0)
    verticals, live_vert, slashes, live_slash = take(vertical), take(vert_count), take(slash), take(slash_count)
    key_block = jnp.arange(blocks, dtype=jnp.int32)
    own = blocks - stretch + jnp.arange(lanes, dtype=jnp.int32)
    chosen = jnp.where(jnp.arange(verticals.shape[1]) < live_vert[:, None], verticals, -1)
    vert_hit = jnp.any(chosen[:, None, :] == key_block[None, :, None], axis=2)
    offset = jnp.where(jnp.arange(slashes.shape[1]) < live_slash[:, None], slashes + 1, 0)
    distance = own[None, :] - key_block[:, None]
    slash_hit = jnp.any(offset[:, :, None, None] == distance[None, None], axis=1)
    allowed = (distance == 0)[None] | ((distance > 0)[None] & (vert_hit[:, :, None] | slash_hit))
    return jnp.where(allowed, 0.0, HIDE).astype(jnp.float32)


def body(queries, keys, values, vertical, vert_count, slash, slash_count):
    seq_count = lax.axis_size("seq")
    position = lax.axis_index("seq")
    query_rows = queries.shape[0]
    key_rows = keys.shape[0]
    sharers = seq_count // KV_HEADS
    piece_rows = key_rows // sharers
    heads = QUERY_HEADS // seq_count
    groups = math.gcd(GROUPS, heads)
    per_group = heads // groups

    def cut(x):
        return x.reshape(sharers, piece_rows, KV_HEADS, HEAD_DIM).transpose(2, 0, 1, 3).reshape(seq_count, piece_rows, HEAD_DIM)

    cache = lax.all_to_all(jnp.concatenate([cut(keys), cut(values)], axis=2), "seq", split_axis=0, concat_axis=0, tiled=True)
    grid = queries.reshape(query_rows, seq_count, groups, per_group * HEAD_DIM)
    asked = [
        lax.all_to_all(grid[:, :, g].transpose(1, 0, 2), "seq", split_axis=0, concat_axis=0, tiled=True).reshape(
            seq_count * query_rows, per_group * HEAD_DIM
        )
        for g in range(groups)
    ]
    cache = [cache]
    for level in range(sharers.bit_length() - 1):
        cache = cache + [swapped(x, "seq", level) for x in cache]
    table = mask_table(
        position * heads, heads, seq_count * key_rows // BLOCK, seq_count * query_rows // BLOCK,
        vertical, vert_count, slash, slash_count,
    )
    side = (position % sharers).astype(jnp.int32).reshape(1)
    answers = []
    for g in range(groups):
        found = attention(asked[g], cache, table[g * per_group:(g + 1) * per_group], side)
        answers.append(
            lax.all_to_all(
                found.reshape(seq_count, query_rows, per_group * HEAD_DIM), "seq", split_axis=0, concat_axis=0, tiled=True
            )
        )
    return jnp.stack(answers, axis=1).transpose(2, 0, 1, 3).reshape(query_rows, QUERY_HEADS * HEAD_DIM)


def solution(mesh):
    return jax.shard_map(
        body,
        mesh=mesh,
        in_specs=(
            P(("rep", "seq"), None),
            P(("rep", "seq"), None),
            P(("rep", "seq"), None),
            P("rep", None),
            P("rep"),
            P("rep", None),
            P("rep"),
        ),
        out_specs=P(("rep", "seq"), None),
        check_vma=False,
    )
```

```python
import functools
import math

import jax
import jax.numpy as jnp
from jax import lax
from jax.experimental import pallas as pl
from jax.experimental.pallas import tpu as pltpu
from jax.sharding import PartitionSpec as P


QUERY_HEADS = 64
KV_HEADS = 8
HEAD_DIM = 128
BLOCK = 64
LANES = 128
ONES = 16
HIDE = -1e30
STEPS = 4


def attention_kernel(factor, pieces, side_ref, table_ref, q_ref, *refs):
    cache_refs, (out_ref, keys, values, mask, qa, sa, sb, acc, sem) = refs[:2 * pieces], refs[-9:]
    head, tile = pl.program_id(0), pl.program_id(1)
    tiles = pl.num_programs(1)
    _, senders, piece_rows, _ = keys.shape
    chunk = pieces * piece_rows
    width = HEAD_DIM
    rows = q_ref.shape[0]
    piece_blocks = piece_rows // BLOCK
    copies = [pltpu.make_async_copy(cache_refs[p], keys.at[p], sem.at[p]) for p in range(pieces)]
    copies += [pltpu.make_async_copy(cache_refs[pieces + p], values.at[p], sem.at[pieces + p]) for p in range(pieces)]
    fresh = (head == 0) & (tile == 0)

    @pl.when(fresh)
    def _():
        for copy in copies:
            copy.start()

    @pl.when(tile == 0)
    def _():
        def fill(sender, carry):
            for p in range(pieces):
                block = (sender * pieces + (p ^ side_ref[0])) * piece_blocks
                for b in range(piece_blocks):
                    row = table_ref[0, pl.ds(block + b, 1), :]
                    at = pl.multiple_of(sender * chunk + (p * piece_blocks + b) * BLOCK, BLOCK)
                    mask[pl.ds(at, BLOCK), :] = jnp.broadcast_to(row, (BLOCK, row.shape[1])).astype(jnp.bfloat16)
            return carry

        lax.fori_loop(0, senders, fill, 0)

    qa[:width, :] = q_ref[...].T
    lane_block = lax.broadcasted_iota(jnp.int32, mask.shape[1:] + (rows,), 1) // BLOCK + tile * (rows // BLOCK)
    qa[width:, :] = (lax.broadcasted_iota(jnp.int32, lane_block.shape, 0) == lane_block).astype(jnp.float32).astype(jnp.bfloat16)
    acc[...] = jnp.zeros_like(acc)
    own = senders - tiles + tile
    count = own + 1

    @pl.when(fresh)
    def _():
        for copy in copies:
            copy.wait()

    def where_at(step):
        return jnp.where(step == 0, own, jnp.minimum(step - 1, own))

    def product(step):
        at = where_at(step)
        held = jnp.concatenate([keys[p, at] for p in range(pieces)], axis=0)
        bias = mask[pl.ds(pl.multiple_of(at * chunk, chunk), chunk), :]
        return jnp.dot(jnp.concatenate([held, bias], axis=1), qa[...], preferred_element_type=jnp.float32)

    def top_of(s):
        return jnp.max(s.reshape(chunk // 8, 8, rows), axis=0)

    def score(step, s_ref):
        s = product(step)
        s_ref[...] = s
        return top_of(s)

    def fold(step, s_ref, peak, part):
        top = jnp.maximum(peak, jnp.max(part, axis=0, keepdims=True))
        alpha = jnp.exp2((peak - top) * factor)
        p = jnp.exp2((s_ref[...] - top) * factor).astype(jnp.bfloat16)
        at = where_at(step)
        held = jnp.concatenate([values[i, at] for i in range(pieces)], axis=0)
        held = jnp.concatenate([held.T, jnp.ones((ONES, chunk), jnp.bfloat16)], axis=0)
        acc[...] = acc[...] * alpha + jnp.dot(held, p, preferred_element_type=jnp.float32)
        return top

    s = product(0)
    row = lax.broadcasted_iota(jnp.int32, s.shape, 0)
    row = (row // piece_rows ^ side_ref[0]) * piece_rows + row % piece_rows
    s = jnp.where(row <= lax.broadcasted_iota(jnp.int32, s.shape, 1), s, HIDE)
    sa[...] = s
    peak = jnp.full((1, rows), HIDE, jnp.float32)

    def pair(i, carry):
        peak, part = carry
        part_b = score(2 * i + 1, sb)
        peak = fold(2 * i, sa, peak, part)
        part = score(2 * i + 2, sa)
        peak = fold(2 * i + 1, sb, peak, part_b)
        return peak, part

    peak, part = lax.fori_loop(0, count // 2, pair, (peak, top_of(s)))

    @pl.when(count % 2 == 1)
    def _():
        fold(count - 1, sa, peak, part)

    total = acc[width:width + 1, :]
    out_ref[...] = (acc[:width, :] / total).T.astype(out_ref.dtype)


def attention(q, keys, values, table, side, first=0, place=0, breadth=1, prior=None):
    pieces = len(keys)
    senders, piece_rows, _ = keys[0].shape
    chunk = pieces * piece_rows
    tiles = q.shape[0] // chunk
    context = senders * chunk
    lanes = table.shape[2]
    factor = math.log2(math.e) / math.sqrt(HEAD_DIM)
    pairs = q.shape[0] * context
    priors = [] if prior is None else [prior]
    anywhere = pl.BlockSpec(memory_space=pl.ANY)
    return pl.pallas_call(
        functools.partial(attention_kernel, factor, pieces),
        out_shape=jax.ShapeDtypeStruct((q.shape[0], breadth * HEAD_DIM), jnp.bfloat16),
        grid_spec=pltpu.PrefetchScalarGridSpec(
            num_scalar_prefetch=1,
            grid=(1, tiles),
            in_specs=[
                pl.BlockSpec((1, table.shape[1], lanes), lambda h, t, s: (h, 0, 0)),
                pl.BlockSpec((chunk, HEAD_DIM), lambda h, t, s: (t, h + first)),
            ]
            + [anywhere] * (2 * pieces + len(priors)),
            out_specs=pl.BlockSpec((chunk, HEAD_DIM), lambda h, t, s: (t, h + place)),
            scratch_shapes=[
                pltpu.VMEM((pieces,) + keys[0].shape, jnp.bfloat16),
                pltpu.VMEM((pieces,) + values[0].shape, jnp.bfloat16),
                pltpu.VMEM((context, lanes), jnp.bfloat16),
                pltpu.VMEM((HEAD_DIM + lanes, chunk), jnp.bfloat16),
                pltpu.VMEM((chunk, chunk), jnp.float32),
                pltpu.VMEM((chunk, chunk), jnp.float32),
                pltpu.VMEM((HEAD_DIM + ONES, chunk), jnp.float32),
                pltpu.SemaphoreType.DMA((2 * pieces,)),
            ],
        ),
        compiler_params=pltpu.CompilerParams(
            dimension_semantics=("arbitrary", "arbitrary"), vmem_limit_bytes=67000000
        ),
        cost_estimate=pl.CostEstimate(
            flops=4 * pairs * HEAD_DIM,
            bytes_accessed=4 * q.shape[0] * HEAD_DIM + 4 * pieces * keys[0].size,
            transcendentals=pairs,
        ),
        input_output_aliases={3 + 2 * pieces: 0} if priors else {},
        name="attention",
    )(side, table, q, *keys, *values, *priors)


def pack_cache(x, sharers):
    rows, _ = x.shape
    piece_rows = rows // sharers
    some = KV_HEADS // STEPS

    def kernel(in_ref, out_ref):
        for g in range(some):
            for p in range(sharers):
                out_ref[g * sharers + p] = in_ref[p * piece_rows:(p + 1) * piece_rows, g * HEAD_DIM:(g + 1) * HEAD_DIM]

    return pl.pallas_call(
        kernel,
        out_shape=jax.ShapeDtypeStruct((KV_HEADS * sharers, piece_rows, HEAD_DIM), x.dtype),
        grid=(STEPS,),
        in_specs=[pl.BlockSpec((rows, some * HEAD_DIM), lambda i: (0, i))],
        out_specs=pl.BlockSpec((some * sharers, piece_rows, HEAD_DIM), lambda i: (i, 0, 0)),
        cost_estimate=pl.CostEstimate(flops=16 * x.size, bytes_accessed=4 * x.size, transcendentals=0),
        name="pack_cache",
    )(x)


def pack_queries(queries, devices, sizes):
    rows, width = queries.shape
    heads = sum(sizes)
    some = devices // STEPS

    def kernel(q_ref, *out_refs):
        for d in range(some):
            head = 0
            for size, out_ref in zip(sizes, out_refs):
                at = (d * heads + head) * HEAD_DIM
                out_ref[d] = q_ref[:, at:at + size * HEAD_DIM]
                head += size

    return pl.pallas_call(
        kernel,
        out_shape=[jax.ShapeDtypeStruct((devices, rows, n * HEAD_DIM), queries.dtype) for n in sizes],
        grid=(STEPS,),
        in_specs=[pl.BlockSpec((rows, width // STEPS), lambda i: (0, i))],
        out_specs=[pl.BlockSpec((some, rows, n * HEAD_DIM), lambda i: (i, 0, 0)) for n in sizes],
        cost_estimate=pl.CostEstimate(flops=16 * queries.size, bytes_accessed=4 * queries.size, transcendentals=0),
        name="pack_queries",
    )(queries)


def unpack_answers(answers):
    devices, rows, _ = answers[0].shape
    sizes = [x.shape[2] // HEAD_DIM for x in answers]
    heads = sum(sizes)
    some = devices // STEPS
    width = devices * heads * HEAD_DIM

    def kernel(*refs):
        out_ref = refs[-1]
        for d in range(some):
            head = 0
            for size, in_ref in zip(sizes, refs):
                at = (d * heads + head) * HEAD_DIM
                out_ref[:, at:at + size * HEAD_DIM] = in_ref[d]
                head += size

    return pl.pallas_call(
        kernel,
        out_shape=jax.ShapeDtypeStruct((rows, width), answers[0].dtype),
        grid=(STEPS,),
        in_specs=[pl.BlockSpec((some, rows, n * HEAD_DIM), lambda i: (i, 0, 0)) for n in sizes],
        out_specs=pl.BlockSpec((rows, width // STEPS), lambda i: (0, i)),
        name="unpack_answers",
    )(*answers)


def swapped(x, axis, bit):
    return lax.ppermute(x, axis, [(i, i ^ 1 << bit) for i in range(lax.axis_size(axis))])


def exchanged(x):
    return lax.all_to_all(x, "seq", split_axis=0, concat_axis=0, tiled=True)


def mask_table(first, heads, blocks, stretch, vertical, vert_count, slash, slash_count):
    lanes = -(-stretch // LANES) * LANES
    take = lambda x: lax.dynamic_slice_in_dim(x, first, heads, 0)
    verticals, live_vert, slashes, live_slash = take(vertical), take(vert_count), take(slash), take(slash_count)
    key_block = jnp.arange(blocks, dtype=jnp.int32)
    own = blocks - stretch + jnp.arange(lanes, dtype=jnp.int32)
    chosen = jnp.where(jnp.arange(verticals.shape[1]) < live_vert[:, None], verticals, -1)
    vert_hit = jnp.any(chosen[:, None, :] == key_block[None, :, None], axis=2)
    offset = jnp.where(jnp.arange(slashes.shape[1]) < live_slash[:, None], slashes + 1, 0)
    distance = own[None, :] - key_block[:, None]
    slash_hit = jnp.any(offset[:, :, None, None] == distance[None, None], axis=1)
    allowed = (distance == 0)[None] | ((distance > 0)[None] & (vert_hit[:, :, None] | slash_hit))
    return jnp.where(allowed, 0.0, HIDE).astype(jnp.float32)


def asked_sizes(heads):
    return (1, 1, heads - 2) if heads > 2 else (1,) * heads


def answer_sizes(heads):
    return (heads - 2, 1, 1) if heads > 2 else (1,) * heads


def body(queries, keys, values, vertical, vert_count, slash, slash_count):
    seq_count = lax.axis_size("seq")
    position = lax.axis_index("seq")
    query_rows = queries.shape[0]
    key_rows = keys.shape[0]
    sharers = seq_count // KV_HEADS
    heads = QUERY_HEADS // seq_count

    def shared(x):
        pieces = [x]
        for level in range(sharers.bit_length() - 1):
            pieces = pieces + [swapped(y, "seq", level) for y in pieces]
        return pieces

    own_keys = exchanged(pack_cache(keys, sharers))
    all_keys = shared(own_keys)
    own_values = exchanged(pack_cache(values, sharers))
    all_values = shared(own_values)
    packed = pack_queries(queries, seq_count, asked_sizes(heads))
    asked = []
    for size, part in zip(asked_sizes(heads), packed):
        part = exchanged(part).reshape(seq_count * query_rows, -1)
        asked += [(part, h) for h in range(size)]
    table = mask_table(
        position * heads, heads, seq_count * key_rows // BLOCK, seq_count * query_rows // BLOCK,
        vertical, vert_count, slash, slash_count,
    )
    side = (position % sharers).astype(jnp.int32).reshape(1)
    tables = [table[h][None] for h in range(heads)]
    answers = []
    head = 0
    for size in answer_sizes(heads):
        found = None
        for place in range(size):
            part, h = asked[head]
            found = attention(part, all_keys, all_values, tables[head], side, h, place, size, found)
            head += 1
        answers.append(exchanged(found.reshape(seq_count, query_rows, size * HEAD_DIM)))
    return unpack_answers(answers)


def solution(mesh):
    return jax.shard_map(
        body,
        mesh=mesh,
        in_specs=(
            P(("rep", "seq"), None),
            P(("rep", "seq"), None),
            P(("rep", "seq"), None),
            P("rep", None),
            P("rep"),
            P("rep", None),
            P("rep"),
        ),
        out_specs=P(("rep", "seq"), None),
        check_vma=False,
    )
```

```python
import functools
import math

import jax
import jax.numpy as jnp
from jax import lax
from jax.experimental import pallas as pl
from jax.experimental.pallas import tpu as pltpu
from jax.sharding import PartitionSpec as P


QUERY_HEADS = 64
KV_HEADS = 8
HEAD_DIM = 128
BLOCK = 64
LANES = 128
ONES = 16
HIDE = -1e30
STEPS = 4
SPAN = 4
GROUP = 8


def attention_kernel(factor, pieces, first, place, steps_ref, list_ref, table_hbm, q_hbm, *refs):
    cache_refs, out_hbm, scratch = refs[:2 * pieces], refs[-13], refs[-12:]
    keys, values, table, q, out, qa, s_even, s_odd, acc, fetch_sem, out_sem, cache_sem = scratch
    width = HEAD_DIM
    rows = SPAN * BLOCK
    chunk = GROUP * BLOCK
    lanes = table.shape[1]
    blocks = keys.shape[0] // BLOCK - 1
    tiles = q.shape[0] // rows
    length = list_ref.shape[0] // tiles
    piece_size = blocks * BLOCK // pieces
    both = range(2)

    fetches = [
        pltpu.make_async_copy(table_hbm, table, fetch_sem.at[0]),
        pltpu.make_async_copy(q_hbm.at[:, first * width:(first + 1) * width], q, fetch_sem.at[1]),
    ]
    loads = []
    for n, (home, cached) in enumerate(((keys, cache_refs[:pieces]), (values, cache_refs[pieces:]))):
        for p in range(pieces):
            loads.append(
                pltpu.make_async_copy(cached[p], home.at[pl.ds(p * piece_size, piece_size)], cache_sem.at[n * pieces + p])
            )
    for copy in fetches + loads:
        copy.start()
    for home in (keys, values):
        home[blocks * BLOCK:, :] = jnp.zeros((BLOCK, width), home.dtype)
    for copy in fetches:
        copy.wait()

    def prepare(tile, carry):
        qa[tile, :width, :] = q[pl.ds(pl.multiple_of(tile * rows, rows), rows), :].T
        column_block = lax.broadcasted_iota(jnp.int32, (lanes, rows), 1) // BLOCK + tile * SPAN
        chosen = lax.broadcasted_iota(jnp.int32, (lanes, rows), 0) == column_block
        qa[tile, width:, :] = chosen.astype(jnp.float32).astype(jnp.bfloat16)
        return carry

    lax.fori_loop(0, tiles, prepare, 0)
    for copy in loads:
        copy.wait()

    def sent(couple):
        where = pl.ds(pl.multiple_of(couple * 2 * rows, 2 * rows), 2 * rows)
        return pltpu.make_async_copy(out.at[where], out_hbm.at[where, place * width:(place + 1) * width], out_sem.at[couple])

    def serve(couple, carry):
        def entries(x, step):
            at = (couple * 2 + x) * length + step * GROUP
            return [list_ref[at + b] for b in range(GROUP)]

        def gathered(home, x, step):
            return jnp.concatenate(
                [home[pl.ds(pl.multiple_of(e * BLOCK, BLOCK), BLOCK), :] for e in entries(x, step)], axis=0
            )

        def product(x, step):
            bias = jnp.concatenate(
                [
                    jnp.broadcast_to(table[pl.ds(e, 1), :], (BLOCK, lanes)).astype(jnp.bfloat16)
                    for e in entries(x, step)
                ],
                axis=0,
            )
            left = jnp.concatenate([gathered(keys, x, step), bias], axis=1)
            return jnp.dot(left, qa[couple * 2 + x], preferred_element_type=jnp.float32)

        def top_of(s):
            return jnp.max(s.reshape(chunk // 8, 8, rows), axis=0)

        def score(step, s_ref):
            tops = []
            for x in both:
                s = product(x, step)
                s_ref[x] = s
                tops.append(top_of(s))
            return tuple(tops)

        def fold(step, s_ref, peaks, parts):
            news = []
            for x in both:
                top = jnp.maximum(peaks[x], jnp.max(parts[x], axis=0, keepdims=True))
                alpha = jnp.exp2((peaks[x] - top) * factor)
                p = jnp.exp2((s_ref[x] - top) * factor).astype(jnp.bfloat16)
                held = gathered(values, x, step).T
                held = jnp.concatenate([held, jnp.ones((ONES, chunk), jnp.bfloat16)], axis=0)
                acc[x] = acc[x] * alpha + jnp.dot(held, p, preferred_element_type=jnp.float32)
                news.append(top)
            return tuple(news)

        acc[...] = jnp.zeros_like(acc)
        parts = []
        for x in both:
            s = product(x, 0)
            row = lax.broadcasted_iota(jnp.int32, s.shape, 0)
            column = lax.broadcasted_iota(jnp.int32, s.shape, 1)
            s = jnp.where((row <= column) | (row >= rows), s, HIDE)
            s_even[x] = s
            parts.append(top_of(s))
        peaks = (jnp.full((1, rows), HIDE, jnp.float32),) * 2
        count = jnp.maximum(steps_ref[couple * 2], steps_ref[couple * 2 + 1])

        def pair(i, carry):
            peaks, parts = carry
            parts_odd = score(2 * i + 1, s_odd)
            peaks = fold(2 * i, s_even, peaks, parts)
            parts = score(2 * i + 2, s_even)
            peaks = fold(2 * i + 1, s_odd, peaks, parts_odd)
            return peaks, parts

        peaks, parts = lax.fori_loop(0, count // 2, pair, (peaks, tuple(parts)))

        @pl.when(count % 2 == 1)
        def _():
            fold(count - 1, s_even, peaks, parts)

        for x in both:
            answer = acc[x, :width, :] / acc[x, width:width + 1, :]
            at = pl.multiple_of((couple * 2 + x) * rows, rows)
            out[pl.ds(at, rows), :] = answer.T.astype(out.dtype)
        sent(couple).start()
        return carry

    lax.fori_loop(0, tiles // 2, serve, 0)

    def drain(couple, carry):
        sent(couple).wait()
        return carry

    lax.fori_loop(0, tiles // 2, drain, 0)


def attention(q, keys, values, table, entries, steps, first=0, place=0, breadth=1, prior=None):
    pieces = len(keys)
    keys, values = [[x.reshape(-1, HEAD_DIM) for x in some] for some in (keys, values)]
    context = pieces * keys[0].shape[0]
    lanes = table.shape[1]
    rows = SPAN * BLOCK
    chunk = GROUP * BLOCK
    tiles = q.shape[0] // rows
    factor = math.log2(math.e) / math.sqrt(HEAD_DIM)
    pairs = q.shape[0] * context
    priors = [] if prior is None else [prior]
    anywhere = pl.BlockSpec(memory_space=pl.ANY)
    scalars = pl.BlockSpec(memory_space=pltpu.SMEM)
    return pl.pallas_call(
        functools.partial(attention_kernel, factor, pieces, first, place),
        out_shape=jax.ShapeDtypeStruct((q.shape[0], breadth * HEAD_DIM), jnp.bfloat16),
        in_specs=[scalars, scalars] + [anywhere] * (2 + 2 * pieces + len(priors)),
        out_specs=anywhere,
        scratch_shapes=[
            pltpu.VMEM((context + BLOCK, HEAD_DIM), jnp.bfloat16),
            pltpu.VMEM((context + BLOCK, HEAD_DIM), jnp.bfloat16),
            pltpu.VMEM(table.shape, jnp.float32),
            pltpu.VMEM((q.shape[0], HEAD_DIM), jnp.bfloat16),
            pltpu.VMEM((q.shape[0], HEAD_DIM), jnp.bfloat16),
            pltpu.VMEM((tiles, HEAD_DIM + lanes, rows), jnp.bfloat16),
            pltpu.VMEM((2, chunk, rows), jnp.float32),
            pltpu.VMEM((2, chunk, rows), jnp.float32),
            pltpu.VMEM((2, HEAD_DIM + ONES, rows), jnp.float32),
            pltpu.SemaphoreType.DMA((2,)),
            pltpu.SemaphoreType.DMA((tiles // 2,)),
            pltpu.SemaphoreType.DMA((2 * pieces,)),
        ],
        compiler_params=pltpu.CompilerParams(vmem_limit_bytes=67000000),
        cost_estimate=pl.CostEstimate(
            flops=4 * pairs * HEAD_DIM,
            bytes_accessed=4 * q.shape[0] * HEAD_DIM + 4 * pieces * keys[0].size,
            transcendentals=pairs,
        ),
        input_output_aliases={4 + 2 * pieces: 0} if priors else {},
        name="attention",
    )(steps, entries, table, q, *keys, *values, *priors)


def make_plan(natural, where_is, heads_at, heads, stretch, vertical, vert_count, slash, slash_count):
    blocks = natural.shape[0]
    lanes = -(-stretch // LANES) * LANES
    tiles = stretch // SPAN
    take = lambda x: lax.dynamic_slice_in_dim(x, heads_at, heads, 0)
    verticals, live_vert, slashes, live_slash = take(vertical), take(vert_count), take(slash), take(slash_count)
    lane = jnp.arange(lanes, dtype=jnp.int32)
    tile = jnp.arange(tiles, dtype=jnp.int32)
    index = jnp.arange(blocks, dtype=jnp.int32)
    distance = blocks - stretch + lane[None, :] - natural[:, None]
    chosen = jnp.where(jnp.arange(verticals.shape[1]) < live_vert[:, None], verticals, -1)
    vert_hit = jnp.any(chosen[:, None, :] == natural[None, :, None], axis=2)
    offset = jnp.where(jnp.arange(slashes.shape[1]) < live_slash[:, None], slashes + 1, 0)
    slash_hit = jnp.any(offset[:, :, None, None] == distance[None, None], axis=1)
    allowed = (distance == 0)[None] | ((distance > 0)[None] & (vert_hit[:, :, None] | slash_hit))
    table = jnp.where(allowed, 0.0, HIDE).astype(jnp.float32)
    table = jnp.pad(table, ((0, 0), (0, 8), (0, 0)), constant_values=HIDE)

    member = (lane[None, :] // SPAN == tile[:, None]).astype(jnp.bfloat16)
    hits = jnp.einsum("hjl,tl->htj", allowed.astype(jnp.bfloat16), member, preferred_element_type=jnp.float32)
    own = blocks - stretch + tile * SPAN
    needed = (hits > 0) & (natural[None, None, :] < own[None, :, None])
    before = (index[:, None] < index[None, :]).astype(jnp.bfloat16)
    rank = jnp.einsum("htj,jk->htk", needed.astype(jnp.bfloat16), before, preferred_element_type=jnp.float32)
    rank = jnp.where(needed, rank.astype(jnp.int32) + SPAN, -1)
    spot = jnp.arange(blocks + 2 * GROUP, dtype=jnp.int32)
    hit = rank[:, :, None, :] == spot[None, None, :, None]
    entries = jnp.min(jnp.where(hit, index[None, None, None, :], blocks), axis=3)
    mine = where_is(jnp.minimum(own[:, None] + spot[None, :], blocks - 1))
    entries = jnp.where(spot < SPAN, mine[None], entries)
    steps = (jnp.sum(needed, axis=2, dtype=jnp.int32) + SPAN + GROUP - 1) // GROUP
    return table, entries.astype(jnp.int32), steps.astype(jnp.int32)


def traded(index):
    return index & ~3 | (index & 1) << 1 | (index >> 1) & 1


def seat(index, flip):
    return jnp.where(flip == 1, traded(index), index)


def pack_cache(x, sharers, flip):
    rows, _ = x.shape
    piece_rows = rows // sharers
    some = KV_HEADS // STEPS

    def kernel(flip_ref, in_ref, out_ref):
        for g in range(some):
            for p in range(sharers):
                out_ref[seat(g * sharers + p, flip_ref[0])] = in_ref[p * piece_rows:(p + 1) * piece_rows, g * HEAD_DIM:(g + 1) * HEAD_DIM]

    return pl.pallas_call(
        kernel,
        out_shape=jax.ShapeDtypeStruct((KV_HEADS * sharers, piece_rows, HEAD_DIM), x.dtype),
        grid_spec=pltpu.PrefetchScalarGridSpec(
            num_scalar_prefetch=1,
            grid=(STEPS,),
            in_specs=[pl.BlockSpec((rows, some * HEAD_DIM), lambda i, s: (0, i))],
            out_specs=pl.BlockSpec((some * sharers, piece_rows, HEAD_DIM), lambda i, s: (i, 0, 0)),
        ),
        cost_estimate=pl.CostEstimate(flops=16 * x.size, bytes_accessed=4 * x.size, transcendentals=0),
        name="pack_cache",
    )(flip, x)


def pack_queries(queries, devices, sizes, flip):
    rows, width = queries.shape
    heads = sum(sizes)
    some = devices // STEPS

    def kernel(flip_ref, q_ref, *out_refs):
        for d in range(some):
            head = 0
            for size, out_ref in zip(sizes, out_refs):
                at = (d * heads + head) * HEAD_DIM
                out_ref[seat(d, flip_ref[0])] = q_ref[:, at:at + size * HEAD_DIM]
                head += size

    return pl.pallas_call(
        kernel,
        out_shape=[jax.ShapeDtypeStruct((devices, rows, n * HEAD_DIM), queries.dtype) for n in sizes],
        grid_spec=pltpu.PrefetchScalarGridSpec(
            num_scalar_prefetch=1,
            grid=(STEPS,),
            in_specs=[pl.BlockSpec((rows, width // STEPS), lambda i, s: (0, i))],
            out_specs=[pl.BlockSpec((some, rows, n * HEAD_DIM), lambda i, s: (i, 0, 0)) for n in sizes],
        ),
        cost_estimate=pl.CostEstimate(flops=16 * queries.size, bytes_accessed=4 * queries.size, transcendentals=0),
        name="pack_queries",
    )(flip, queries)


def unpack_answers(answers, flip):
    devices, rows, _ = answers[0].shape
    sizes = [x.shape[2] // HEAD_DIM for x in answers]
    heads = sum(sizes)
    some = devices // STEPS
    width = devices * heads * HEAD_DIM

    def kernel(flip_ref, *refs):
        out_ref = refs[-1]
        for d in range(some):
            head = 0
            for size, in_ref in zip(sizes, refs):
                at = (d * heads + head) * HEAD_DIM
                out_ref[:, at:at + size * HEAD_DIM] = in_ref[seat(d, flip_ref[0])]
                head += size

    return pl.pallas_call(
        kernel,
        out_shape=jax.ShapeDtypeStruct((rows, width), answers[0].dtype),
        grid_spec=pltpu.PrefetchScalarGridSpec(
            num_scalar_prefetch=1,
            grid=(STEPS,),
            in_specs=[pl.BlockSpec((some, rows, n * HEAD_DIM), lambda i, s: (i, 0, 0)) for n in sizes],
            out_specs=pl.BlockSpec((rows, width // STEPS), lambda i, s: (0, i)),
        ),
        name="unpack_answers",
    )(flip, *answers)


def swapped(x, bit):
    count = lax.axis_size("seq")
    moves = []
    for rep in range(lax.axis_size("rep")):
        turn = traded if rep % 2 else int
        moves += [(rep * count + i, rep * count + turn(turn(i) ^ 1 << bit)) for i in range(count)]
    return lax.ppermute(x, ("rep", "seq"), moves)


def exchanged(x):
    return lax.all_to_all(x, "seq", split_axis=0, concat_axis=0, tiled=True)


def asked_sizes(heads):
    return (1, 1, heads - 2) if heads > 2 else (1,) * heads


def answer_sizes(heads):
    return (heads - 2, 1, 1) if heads > 2 else (1,) * heads


def body(queries, keys, values, vertical, vert_count, slash, slash_count):
    seq_count = lax.axis_size("seq")
    flip = (lax.axis_index("rep") % 2).astype(jnp.int32).reshape(1)
    position = seat(lax.axis_index("seq"), flip[0])
    query_rows = queries.shape[0]
    key_rows = keys.shape[0]
    sharers = seq_count // KV_HEADS
    heads = QUERY_HEADS // seq_count

    def shared(x):
        pieces = [x]
        for level in range(sharers.bit_length() - 1):
            pieces = pieces + [swapped(y, level) for y in pieces]
        return pieces

    own_keys = exchanged(pack_cache(keys, sharers, flip))
    all_keys = shared(own_keys)
    own_values = exchanged(pack_cache(values, sharers, flip))
    all_values = shared(own_values)
    packed = pack_queries(queries, seq_count, asked_sizes(heads), flip)
    asked = []
    for size, part in zip(asked_sizes(heads), packed):
        part = exchanged(part).reshape(seq_count * query_rows, -1)
        asked += [(part, h) for h in range(size)]
    piece_blocks = key_rows // sharers // BLOCK
    side = position % sharers
    spot = jnp.arange(seq_count * key_rows // BLOCK, dtype=jnp.int32)
    piece = spot // (seq_count * piece_blocks)
    sender = spot // piece_blocks % seq_count
    natural = (sender * sharers + (piece ^ side)) * piece_blocks + spot % piece_blocks

    def where_is(block):
        piece = block // piece_blocks % sharers ^ side
        return (piece * seq_count + block // (piece_blocks * sharers)) * piece_blocks + block % piece_blocks

    table, entries, steps = make_plan(
        natural, where_is, position * heads, heads, seq_count * query_rows // BLOCK,
        vertical, vert_count, slash, slash_count,
    )
    plans = [(table[h], entries[h].reshape(-1), steps[h]) for h in range(heads)]
    answers = []
    head = 0
    for size in answer_sizes(heads):
        found = None
        for place in range(size):
            part, h = asked[head]
            found = attention(part, all_keys, all_values, *plans[head], h, place, size, found)
            head += 1
        answers.append(exchanged(found.reshape(seq_count, query_rows, size * HEAD_DIM)))
    return unpack_answers(answers, flip)


def solution(mesh):
    return jax.shard_map(
        body,
        mesh=mesh,
        in_specs=(
            P(("rep", "seq"), None),
            P(("rep", "seq"), None),
            P(("rep", "seq"), None),
            P("rep", None),
            P("rep"),
            P("rep", None),
            P("rep"),
        ),
        out_specs=P(("rep", "seq"), None),
        check_vma=False,
    )
```

```python
import functools
import math

import jax
import jax.numpy as jnp
from jax import lax
from jax.experimental import pallas as pl
from jax.experimental.pallas import tpu as pltpu
from jax.sharding import PartitionSpec as P


QUERY_HEADS = 64
KV_HEADS = 8
HEAD_DIM = 128
BLOCK = 64
LANES = 128
ONES = 16
HIDE = -1e30
STEPS = 4
SPAN = 4
PHASES = (2, 0, 1, 3)
GROUP = 12


def attention_kernel(factor, pieces, first, place, steps_ref, list_ref, table_hbm, q_hbm, *refs):
    cache_refs, out_hbm, scratch = refs[:2 * pieces], refs[-13], refs[-12:]
    keys, values, table, q, out, qa, s_even, s_odd, acc, fetch_sem, out_sem, cache_sem = scratch
    width = HEAD_DIM
    rows = SPAN * BLOCK
    chunk = GROUP * BLOCK
    lanes = table.shape[1]
    blocks = keys.shape[0] // BLOCK - 1
    tiles = q.shape[0] // rows
    length = list_ref.shape[0] // tiles
    piece_size = blocks * BLOCK // pieces
    both = range(2)

    fetches = [
        pltpu.make_async_copy(table_hbm, table, fetch_sem.at[0]),
        pltpu.make_async_copy(q_hbm.at[:, first * width:(first + 1) * width], q, fetch_sem.at[1]),
    ]
    loads = []
    for n, (home, cached) in enumerate(((keys, cache_refs[:pieces]), (values, cache_refs[pieces:]))):
        for p in range(pieces):
            loads.append(
                pltpu.make_async_copy(cached[p], home.at[pl.ds(p * piece_size, piece_size)], cache_sem.at[n * pieces + p])
            )
    for copy in fetches + loads:
        copy.start()
    for home in (keys, values):
        home[blocks * BLOCK:, :] = jnp.zeros((BLOCK, width), home.dtype)
    for copy in fetches:
        copy.wait()

    def prepare(tile, carry):
        qa[tile, :width, :] = q[pl.ds(pl.multiple_of(tile * rows, rows), rows), :].T
        column_block = lax.broadcasted_iota(jnp.int32, (lanes, rows), 1) // BLOCK + tile * SPAN
        chosen = lax.broadcasted_iota(jnp.int32, (lanes, rows), 0) == column_block
        qa[tile, width:, :] = chosen.astype(jnp.float32).astype(jnp.bfloat16)
        return carry

    lax.fori_loop(0, tiles, prepare, 0)
    for copy in loads[:pieces]:
        copy.wait()

    def sent(couple):
        where = pl.ds(pl.multiple_of(couple * 2 * rows, 2 * rows), 2 * rows)
        return pltpu.make_async_copy(out.at[where], out_hbm.at[where, place * width:(place + 1) * width], out_sem.at[couple])

    def serve(couple, carry):
        def entries(x, step):
            at = (couple * 2 + x) * length + step * GROUP
            return [list_ref[at + b] for b in range(GROUP)]

        def gathered(home, x, step):
            return jnp.concatenate(
                [home[pl.ds(pl.multiple_of(e * BLOCK, BLOCK), BLOCK), :] for e in entries(x, step)], axis=0
            )

        def product(x, step):
            bias = jnp.concatenate(
                [
                    jnp.broadcast_to(table[pl.ds(e, 1), :], (BLOCK, lanes)).astype(jnp.bfloat16)
                    for e in entries(x, step)
                ],
                axis=0,
            )
            left = jnp.concatenate([gathered(keys, x, step), bias], axis=1)
            return jnp.dot(left, qa[couple * 2 + x], preferred_element_type=jnp.float32)

        def top_of(s):
            return jnp.max(s.reshape(chunk // 8, 8, rows), axis=0)

        def score(step, s_ref):
            tops = []
            for x in both:
                s = product(x, step)
                s_ref[x] = s
                tops.append(top_of(s))
            return tuple(tops)

        def fold(step, s_ref, peaks, parts):
            news = []
            for x in both:
                top = jnp.maximum(peaks[x], jnp.max(parts[x], axis=0, keepdims=True))
                alpha = jnp.exp2((peaks[x] - top) * factor)
                p = jnp.exp2((s_ref[x] - top) * factor).astype(jnp.bfloat16)
                held = gathered(values, x, step).T
                held = jnp.concatenate([held, jnp.ones((ONES, chunk), jnp.bfloat16)], axis=0)
                acc[x] = acc[x] * alpha + jnp.dot(held, p, preferred_element_type=jnp.float32)
                news.append(top)
            return tuple(news)

        acc[...] = jnp.zeros_like(acc)
        parts = []
        for x in both:
            s = product(x, 0)
            row = lax.broadcasted_iota(jnp.int32, s.shape, 0)
            column = lax.broadcasted_iota(jnp.int32, s.shape, 1)
            s = jnp.where((row <= column) | (row >= rows), s, HIDE)
            s_even[x] = s
            parts.append(top_of(s))

        @pl.when(couple == 0)
        def _():
            for copy in loads[pieces:]:
                copy.wait()

        peaks = (jnp.full((1, rows), HIDE, jnp.float32),) * 2
        count = jnp.maximum(steps_ref[couple * 2], steps_ref[couple * 2 + 1])

        def pair(i, carry):
            peaks, parts = carry
            parts_odd = score(2 * i + 1, s_odd)
            peaks = fold(2 * i, s_even, peaks, parts)
            parts = score(2 * i + 2, s_even)
            peaks = fold(2 * i + 1, s_odd, peaks, parts_odd)
            return peaks, parts

        peaks, parts = lax.fori_loop(0, count // 2, pair, (peaks, tuple(parts)))

        @pl.when(count % 2 == 1)
        def _():
            fold(count - 1, s_even, peaks, parts)

        for x in both:
            answer = acc[x, :width, :] / acc[x, width:width + 1, :]
            at = pl.multiple_of((couple * 2 + x) * rows, rows)
            out[pl.ds(at, rows), :] = answer.T.astype(out.dtype)
        sent(couple).start()
        return carry

    lax.fori_loop(0, tiles // 2, serve, 0)

    def drain(couple, carry):
        sent(couple).wait()
        return carry

    lax.fori_loop(0, tiles // 2, drain, 0)


def attention(q, keys, values, table, entries, steps, first=0, place=0, breadth=1, prior=None):
    pieces = len(keys)
    keys, values = [[x.reshape(-1, HEAD_DIM) for x in some] for some in (keys, values)]
    context = pieces * keys[0].shape[0]
    lanes = table.shape[1]
    rows = SPAN * BLOCK
    chunk = GROUP * BLOCK
    tiles = q.shape[0] // rows
    factor = math.log2(math.e) / math.sqrt(HEAD_DIM)
    pairs = q.shape[0] * context
    priors = [] if prior is None else [prior]
    anywhere = pl.BlockSpec(memory_space=pl.ANY)
    scalars = pl.BlockSpec(memory_space=pltpu.SMEM)
    return pl.pallas_call(
        functools.partial(attention_kernel, factor, pieces, first, place),
        out_shape=jax.ShapeDtypeStruct((q.shape[0], breadth * HEAD_DIM), jnp.bfloat16),
        in_specs=[scalars, scalars] + [anywhere] * (2 + 2 * pieces + len(priors)),
        out_specs=anywhere,
        scratch_shapes=[
            pltpu.VMEM((context + BLOCK, HEAD_DIM), jnp.bfloat16),
            pltpu.VMEM((context + BLOCK, HEAD_DIM), jnp.bfloat16),
            pltpu.VMEM(table.shape, jnp.float32),
            pltpu.VMEM((q.shape[0], HEAD_DIM), jnp.bfloat16),
            pltpu.VMEM((q.shape[0], HEAD_DIM), jnp.bfloat16),
            pltpu.VMEM((tiles, HEAD_DIM + lanes, rows), jnp.bfloat16),
            pltpu.VMEM((2, chunk, rows), jnp.float32),
            pltpu.VMEM((2, chunk, rows), jnp.float32),
            pltpu.VMEM((2, HEAD_DIM + ONES, rows), jnp.float32),
            pltpu.SemaphoreType.DMA((2,)),
            pltpu.SemaphoreType.DMA((tiles // 2,)),
            pltpu.SemaphoreType.DMA((2 * pieces,)),
        ],
        compiler_params=pltpu.CompilerParams(vmem_limit_bytes=67000000),
        cost_estimate=pl.CostEstimate(
            flops=4 * pairs * HEAD_DIM,
            bytes_accessed=4 * q.shape[0] * HEAD_DIM + 4 * pieces * keys[0].size,
            transcendentals=pairs,
        ),
        input_output_aliases={4 + 2 * pieces: 0} if priors else {},
        name="attention",
    )(steps, entries, table, q, *keys, *values, *priors)


def make_plan(natural, where_is, chosen_heads, stretch, vertical, vert_count, slash, slash_count):
    blocks = natural.shape[0]
    lanes = -(-stretch // LANES) * LANES
    tiles = stretch // SPAN
    take = lambda x: x[chosen_heads]
    verticals, live_vert, slashes, live_slash = take(vertical), take(vert_count), take(slash), take(slash_count)
    lane = jnp.arange(lanes, dtype=jnp.int32)
    tile = jnp.arange(tiles, dtype=jnp.int32)
    index = jnp.arange(blocks, dtype=jnp.int32)
    distance = blocks - stretch + lane[None, :] - natural[:, None]
    chosen = jnp.where(jnp.arange(verticals.shape[1]) < live_vert[:, None], verticals, -1)
    vert_hit = jnp.any(chosen[:, None, :] == natural[None, :, None], axis=2)
    offset = jnp.where(jnp.arange(slashes.shape[1]) < live_slash[:, None], slashes + 1, 0)
    slash_hit = jnp.any(offset[:, :, None, None] == distance[None, None], axis=1)
    allowed = (distance == 0)[None] | ((distance > 0)[None] & (vert_hit[:, :, None] | slash_hit))
    table = jnp.where(allowed, 0.0, HIDE).astype(jnp.float32)
    table = jnp.pad(table, ((0, 0), (0, 8), (0, 0)), constant_values=HIDE)

    member = (lane[None, :] // SPAN == tile[:, None]).astype(jnp.bfloat16)
    hits = jnp.einsum("hjl,tl->htj", allowed.astype(jnp.bfloat16), member, preferred_element_type=jnp.float32)
    own = blocks - stretch + tile * SPAN
    needed = (hits > 0) & (natural[None, None, :] < own[None, :, None])
    before = (index[:, None] < index[None, :]).astype(jnp.bfloat16)
    rank = jnp.einsum("htj,jk->htk", needed.astype(jnp.bfloat16), before, preferred_element_type=jnp.float32)
    rank = jnp.where(needed, rank.astype(jnp.int32) + SPAN, -1)
    spot = jnp.arange(blocks + 2 * GROUP, dtype=jnp.int32)
    hit = rank[:, :, None, :] == spot[None, None, :, None]
    entries = jnp.min(jnp.where(hit, index[None, None, None, :], blocks), axis=3)
    mine = where_is(jnp.minimum(own[:, None] + spot[None, :], blocks - 1))
    entries = jnp.where(spot < SPAN, mine[None], entries)
    steps = (jnp.sum(needed, axis=2, dtype=jnp.int32) + SPAN + GROUP - 1) // GROUP
    return table, entries.astype(jnp.int32), steps.astype(jnp.int32)


def traded(index):
    return index & ~3 | (index & 1) << 1 | (index >> 1) & 1


def seat(index, flip):
    return jnp.where(flip == 1, traded(index), index)


def pack_cache(x, sharers, flip):
    rows, _ = x.shape
    piece_rows = rows // sharers
    some = KV_HEADS // STEPS

    def kernel(flip_ref, in_ref, out_ref):
        for g in range(some):
            for p in range(sharers):
                out_ref[seat(g * sharers + p, flip_ref[0])] = in_ref[p * piece_rows:(p + 1) * piece_rows, g * HEAD_DIM:(g + 1) * HEAD_DIM]

    return pl.pallas_call(
        kernel,
        out_shape=jax.ShapeDtypeStruct((KV_HEADS * sharers, piece_rows, HEAD_DIM), x.dtype),
        grid_spec=pltpu.PrefetchScalarGridSpec(
            num_scalar_prefetch=1,
            grid=(STEPS,),
            in_specs=[pl.BlockSpec((rows, some * HEAD_DIM), lambda i, s: (0, i))],
            out_specs=pl.BlockSpec((some * sharers, piece_rows, HEAD_DIM), lambda i, s: (i, 0, 0)),
        ),
        cost_estimate=pl.CostEstimate(flops=16 * x.size, bytes_accessed=4 * x.size, transcendentals=0),
        name="pack_cache",
    )(flip, x)


def pack_queries(queries, devices, sizes, flip, order):
    rows, width = queries.shape
    heads = sum(sizes)
    some = devices // STEPS

    def kernel(flip_ref, order_ref, q_ref, *out_refs):
        for d in range(some):
            phase = 0
            for size, out_ref in zip(sizes, out_refs):
                for place in range(size):
                    head = order_ref[(pl.program_id(0) * some + d) * heads + phase]
                    at = pl.multiple_of((d * heads + head) * HEAD_DIM, HEAD_DIM)
                    out_ref[seat(d, flip_ref[0]), :, place * HEAD_DIM:(place + 1) * HEAD_DIM] = q_ref[:, pl.ds(at, HEAD_DIM)]
                    phase += 1

    return pl.pallas_call(
        kernel,
        out_shape=[jax.ShapeDtypeStruct((devices, rows, n * HEAD_DIM), queries.dtype) for n in sizes],
        grid_spec=pltpu.PrefetchScalarGridSpec(
            num_scalar_prefetch=2,
            grid=(STEPS,),
            in_specs=[pl.BlockSpec((rows, width // STEPS), lambda i, s, o: (0, i))],
            out_specs=[pl.BlockSpec((some, rows, n * HEAD_DIM), lambda i, s, o: (i, 0, 0)) for n in sizes],
        ),
        cost_estimate=pl.CostEstimate(flops=16 * queries.size, bytes_accessed=4 * queries.size, transcendentals=0),
        name="pack_queries",
    )(flip, order, queries)


def unpack_answers(answers, flip, order):
    devices, rows, _ = answers[0].shape
    sizes = [x.shape[2] // HEAD_DIM for x in answers]
    heads = sum(sizes)
    some = devices // STEPS
    width = devices * heads * HEAD_DIM

    def kernel(flip_ref, order_ref, *refs):
        out_ref = refs[-1]
        for d in range(some):
            phase = 0
            for size, in_ref in zip(sizes, refs):
                for place in range(size):
                    head = order_ref[(pl.program_id(0) * some + d) * heads + phase]
                    at = pl.multiple_of((d * heads + head) * HEAD_DIM, HEAD_DIM)
                    out_ref[:, pl.ds(at, HEAD_DIM)] = in_ref[seat(d, flip_ref[0]), :, place * HEAD_DIM:(place + 1) * HEAD_DIM]
                    phase += 1

    return pl.pallas_call(
        kernel,
        out_shape=jax.ShapeDtypeStruct((rows, width), answers[0].dtype),
        grid_spec=pltpu.PrefetchScalarGridSpec(
            num_scalar_prefetch=2,
            grid=(STEPS,),
            in_specs=[pl.BlockSpec((some, rows, n * HEAD_DIM), lambda i, s, o: (i, 0, 0)) for n in sizes],
            out_specs=pl.BlockSpec((rows, width // STEPS), lambda i, s, o: (0, i)),
        ),
        name="unpack_answers",
    )(flip, order, *answers)


def swapped(x, bit):
    count = lax.axis_size("seq")
    moves = []
    for rep in range(lax.axis_size("rep")):
        turn = traded if rep % 2 else int
        moves += [(rep * count + i, rep * count + turn(turn(i) ^ 1 << bit)) for i in range(count)]
    return lax.ppermute(x, ("rep", "seq"), moves)


def exchanged(x):
    return lax.all_to_all(x, "seq", split_axis=0, concat_axis=0, tiled=True)


def asked_sizes(heads):
    return (1, 1, heads - 2) if heads > 2 else (1,) * heads


def answer_sizes(heads):
    return (heads - 2, 1, 1) if heads > 2 else (1,) * heads


def served_order(vert_count, slash_count, heads, blocks, stretch):
    free = (1 - vert_count / blocks) * (1 - slash_count / (blocks - stretch)) ** SPAN
    free = free.reshape(-1, heads)
    index = jnp.arange(heads, dtype=jnp.int32)
    mine, other = free[:, :, None], free[:, None, :]
    ahead = (other < mine) | ((other == mine) & (index[None, None, :] < index[None, :, None]))
    rank = jnp.sum(ahead, axis=2, dtype=jnp.int32)
    turns = PHASES if heads == len(PHASES) else range(heads)
    ranks = jnp.stack([jnp.sum(jnp.where(rank == r, index, 0), axis=1) for r in turns], axis=1)
    return ranks.astype(jnp.int32)


def body(queries, keys, values, vertical, vert_count, slash, slash_count):
    seq_count = lax.axis_size("seq")
    flip = (lax.axis_index("rep") % 2).astype(jnp.int32).reshape(1)
    position = seat(lax.axis_index("seq"), flip[0])
    query_rows = queries.shape[0]
    key_rows = keys.shape[0]
    sharers = seq_count // KV_HEADS
    heads = QUERY_HEADS // seq_count

    def shared(x):
        pieces = [x]
        for level in range(sharers.bit_length() - 1):
            pieces = pieces + [swapped(y, level) for y in pieces]
        return pieces

    own_keys = exchanged(pack_cache(keys, sharers, flip))
    all_keys = shared(own_keys)
    own_values = exchanged(pack_cache(values, sharers, flip))
    all_values = shared(own_values)
    blocks, stretch = seq_count * key_rows // BLOCK, seq_count * query_rows // BLOCK
    order = served_order(vert_count, slash_count, heads, blocks, stretch)
    mine = position * heads + lax.dynamic_index_in_dim(order, position, 0, keepdims=False)
    order = order.reshape(-1)
    packed = pack_queries(queries, seq_count, asked_sizes(heads), flip, order)
    asked = []
    for size, part in zip(asked_sizes(heads), packed):
        part = exchanged(part).reshape(seq_count * query_rows, -1)
        asked += [(part, h) for h in range(size)]
    piece_blocks = key_rows // sharers // BLOCK
    side = position % sharers
    spot = jnp.arange(seq_count * key_rows // BLOCK, dtype=jnp.int32)
    piece = spot // (seq_count * piece_blocks)
    sender = spot // piece_blocks % seq_count
    natural = (sender * sharers + (piece ^ side)) * piece_blocks + spot % piece_blocks

    def where_is(block):
        piece = block // piece_blocks % sharers ^ side
        return (piece * seq_count + block // (piece_blocks * sharers)) * piece_blocks + block % piece_blocks

    table, entries, steps = make_plan(
        natural, where_is, mine, stretch,
        vertical, vert_count, slash, slash_count,
    )
    plans = [(table[h], entries[h].reshape(-1), steps[h]) for h in range(heads)]
    answers = []
    head = 0
    for size in answer_sizes(heads):
        found = None
        for place in range(size):
            part, h = asked[head]
            found = attention(part, all_keys, all_values, *plans[head], h, place, size, found)
            head += 1
        answers.append(exchanged(found.reshape(seq_count, query_rows, size * HEAD_DIM)))
    return unpack_answers(answers, flip, order)


def solution(mesh):
    return jax.shard_map(
        body,
        mesh=mesh,
        in_specs=(
            P(("rep", "seq"), None),
            P(("rep", "seq"), None),
            P(("rep", "seq"), None),
            P("rep", None),
            P("rep"),
            P("rep", None),
            P("rep"),
        ),
        out_specs=P(("rep", "seq"), None),
        check_vma=False,
    )
```

```python
import functools
import math

import jax
import jax.numpy as jnp
from jax import lax
from jax.experimental import pallas as pl
from jax.experimental.pallas import tpu as pltpu
from jax.sharding import PartitionSpec as P


QUERY_HEADS = 64
KV_HEADS = 8
HEAD_DIM = 128
BLOCK = 64
LANES = 128
ONES = 16
HIDE = -1e30
STEPS = 2
SPAN = 4
PHASES = (2, 0, 1, 3)
GROUP = 12


def attention_kernel(factor, pieces, first, place, steps_ref, list_ref, table_hbm, q_hbm, *refs):
    cache_refs, out_hbm, scratch = refs[:2 * pieces], refs[-13], refs[-12:]
    keys, values, table, q, out, qa, s_even, s_odd, acc, fetch_sem, out_sem, cache_sem = scratch
    width = HEAD_DIM
    rows = SPAN * BLOCK
    chunk = GROUP * BLOCK
    lanes = table.shape[1]
    blocks = keys.shape[0] // BLOCK - 1
    tiles = q.shape[0] // rows
    length = list_ref.shape[0] // tiles
    piece_size = blocks * BLOCK // pieces
    both = range(2)

    fetches = [
        pltpu.make_async_copy(table_hbm, table, fetch_sem.at[0]),
        pltpu.make_async_copy(q_hbm.at[:, first * width:(first + 1) * width], q, fetch_sem.at[1]),
    ]
    loads = []
    for n, (home, cached) in enumerate(((keys, cache_refs[:pieces]), (values, cache_refs[pieces:]))):
        for p in range(pieces):
            loads.append(
                pltpu.make_async_copy(cached[p], home.at[pl.ds(p * piece_size, piece_size)], cache_sem.at[n * pieces + p])
            )
    for copy in fetches + loads:
        copy.start()
    for home in (keys, values):
        home[blocks * BLOCK:, :] = jnp.zeros((BLOCK, width), home.dtype)
    for copy in fetches:
        copy.wait()

    def prepare(tile, carry):
        qa[tile, :width, :] = q[pl.ds(pl.multiple_of(tile * rows, rows), rows), :].T
        column_block = lax.broadcasted_iota(jnp.int32, (lanes, rows), 1) // BLOCK + tile * SPAN
        chosen = lax.broadcasted_iota(jnp.int32, (lanes, rows), 0) == column_block
        qa[tile, width:, :] = chosen.astype(jnp.float32).astype(jnp.bfloat16)
        return carry

    lax.fori_loop(0, tiles, prepare, 0)
    for copy in loads[:pieces]:
        copy.wait()

    def sent(couple):
        where = pl.ds(pl.multiple_of(couple * 2 * rows, 2 * rows), 2 * rows)
        return pltpu.make_async_copy(out.at[where], out_hbm.at[where, place * width:(place + 1) * width], out_sem.at[couple])

    def serve(couple, carry):
        def entries(x, step):
            at = (couple * 2 + x) * length + step * GROUP
            return [list_ref[at + b] for b in range(GROUP)]

        def gathered(home, x, step):
            return jnp.concatenate(
                [home[pl.ds(pl.multiple_of(e * BLOCK, BLOCK), BLOCK), :] for e in entries(x, step)], axis=0
            )

        def product(x, step):
            bias = jnp.concatenate(
                [
                    jnp.broadcast_to(table[pl.ds(e, 1), :], (BLOCK, lanes)).astype(jnp.bfloat16)
                    for e in entries(x, step)
                ],
                axis=0,
            )
            left = jnp.concatenate([gathered(keys, x, step), bias], axis=1)
            return jnp.dot(left, qa[couple * 2 + x], preferred_element_type=jnp.float32)

        def top_of(s):
            return jnp.max(s.reshape(chunk // 8, 8, rows), axis=0)

        def score(step, s_ref):
            tops = []
            for x in both:
                s = product(x, step)
                s_ref[x] = s
                tops.append(top_of(s))
            return tuple(tops)

        def fold(step, s_ref, peaks, parts):
            news = []
            for x in both:
                top = jnp.maximum(peaks[x], jnp.max(parts[x], axis=0, keepdims=True))
                alpha = jnp.exp2((peaks[x] - top) * factor)
                p = jnp.exp2((s_ref[x] - top) * factor).astype(jnp.bfloat16)
                held = gathered(values, x, step).T
                held = jnp.concatenate([held, jnp.ones((ONES, chunk), jnp.bfloat16)], axis=0)
                acc[x] = acc[x] * alpha + jnp.dot(held, p, preferred_element_type=jnp.float32)
                news.append(top)
            return tuple(news)

        acc[...] = jnp.zeros_like(acc)
        parts = []
        for x in both:
            s = product(x, 0)
            row = lax.broadcasted_iota(jnp.int32, s.shape, 0)
            column = lax.broadcasted_iota(jnp.int32, s.shape, 1)
            s = jnp.where((row <= column) | (row >= rows), s, HIDE)
            s_even[x] = s
            parts.append(top_of(s))

        @pl.when(couple == 0)
        def _():
            for copy in loads[pieces:]:
                copy.wait()

        peaks = (jnp.full((1, rows), HIDE, jnp.float32),) * 2
        count = jnp.maximum(steps_ref[couple * 2], steps_ref[couple * 2 + 1])

        def pair(i, carry):
            peaks, parts = carry
            parts_odd = score(2 * i + 1, s_odd)
            peaks = fold(2 * i, s_even, peaks, parts)
            parts = score(2 * i + 2, s_even)
            peaks = fold(2 * i + 1, s_odd, peaks, parts_odd)
            return peaks, parts

        peaks, parts = lax.fori_loop(0, (count - 1) // 2, pair, (peaks, tuple(parts)))

        @pl.when(count % 2 == 1)
        def _():
            fold(count - 1, s_even, peaks, parts)

        @pl.when(count % 2 == 0)
        def _():
            parts_odd = score(count - 1, s_odd)
            fold(count - 1, s_odd, fold(count - 2, s_even, peaks, parts), parts_odd)

        for x in both:
            answer = acc[x, :width, :] / acc[x, width:width + 1, :]
            at = pl.multiple_of((couple * 2 + x) * rows, rows)
            out[pl.ds(at, rows), :] = answer.T.astype(out.dtype)
        sent(couple).start()
        return carry

    lax.fori_loop(0, tiles // 2, serve, 0)

    def drain(couple, carry):
        sent(couple).wait()
        return carry

    lax.fori_loop(0, tiles // 2, drain, 0)


def attention(q, keys, values, table, entries, steps, first=0, place=0, breadth=1, prior=None):
    pieces = len(keys)
    keys, values = [[x.reshape(-1, HEAD_DIM) for x in some] for some in (keys, values)]
    context = pieces * keys[0].shape[0]
    lanes = table.shape[1]
    rows = SPAN * BLOCK
    chunk = GROUP * BLOCK
    tiles = q.shape[0] // rows
    factor = math.log2(math.e) / math.sqrt(HEAD_DIM)
    pairs = q.shape[0] * context
    priors = [] if prior is None else [prior]
    anywhere = pl.BlockSpec(memory_space=pl.ANY)
    scalars = pl.BlockSpec(memory_space=pltpu.SMEM)
    return pl.pallas_call(
        functools.partial(attention_kernel, factor, pieces, first, place),
        out_shape=jax.ShapeDtypeStruct((q.shape[0], breadth * HEAD_DIM), jnp.bfloat16),
        in_specs=[scalars, scalars] + [anywhere] * (2 + 2 * pieces + len(priors)),
        out_specs=anywhere,
        scratch_shapes=[
            pltpu.VMEM((context + BLOCK, HEAD_DIM), jnp.bfloat16),
            pltpu.VMEM((context + BLOCK, HEAD_DIM), jnp.bfloat16),
            pltpu.VMEM(table.shape, jnp.float32),
            pltpu.VMEM((q.shape[0], HEAD_DIM), jnp.bfloat16),
            pltpu.VMEM((q.shape[0], HEAD_DIM), jnp.bfloat16),
            pltpu.VMEM((tiles, HEAD_DIM + lanes, rows), jnp.bfloat16),
            pltpu.VMEM((2, chunk, rows), jnp.float32),
            pltpu.VMEM((2, chunk, rows), jnp.float32),
            pltpu.VMEM((2, HEAD_DIM + ONES, rows), jnp.float32),
            pltpu.SemaphoreType.DMA((2,)),
            pltpu.SemaphoreType.DMA((tiles // 2,)),
            pltpu.SemaphoreType.DMA((2 * pieces,)),
        ],
        compiler_params=pltpu.CompilerParams(vmem_limit_bytes=67000000),
        cost_estimate=pl.CostEstimate(
            flops=4 * pairs * HEAD_DIM,
            bytes_accessed=4 * q.shape[0] * HEAD_DIM + 4 * pieces * keys[0].size,
            transcendentals=pairs,
        ),
        input_output_aliases={4 + 2 * pieces: 0} if priors else {},
        name="attention",
    )(steps, entries, table, q, *keys, *values, *priors)


def make_plan(natural, where_is, chosen_heads, stretch, vertical, vert_count, slash, slash_count):
    blocks = natural.shape[0]
    lanes = -(-stretch // LANES) * LANES
    tiles = stretch // SPAN
    take = lambda x: x[chosen_heads]
    verticals, live_vert, slashes, live_slash = take(vertical), take(vert_count), take(slash), take(slash_count)
    lane = jnp.arange(lanes, dtype=jnp.int32)
    tile = jnp.arange(tiles, dtype=jnp.int32)
    index = jnp.arange(blocks, dtype=jnp.int32)
    distance = blocks - stretch + lane[None, :] - natural[:, None]
    chosen = jnp.where(jnp.arange(verticals.shape[1]) < live_vert[:, None], verticals, -1)
    vert_hit = jnp.any(chosen[:, None, :] == natural[None, :, None], axis=2)
    offset = jnp.where(jnp.arange(slashes.shape[1]) < live_slash[:, None], slashes + 1, 0)
    slash_hit = jnp.any(offset[:, :, None, None] == distance[None, None], axis=1)
    allowed = (distance == 0)[None] | ((distance > 0)[None] & (vert_hit[:, :, None] | slash_hit))
    table = jnp.where(allowed, 0.0, HIDE).astype(jnp.float32)
    table = jnp.pad(table, ((0, 0), (0, 8), (0, 0)), constant_values=HIDE)

    member = (lane[None, :] // SPAN == tile[:, None]).astype(jnp.bfloat16)
    hits = jnp.einsum("hjl,tl->htj", allowed.astype(jnp.bfloat16), member, preferred_element_type=jnp.float32)
    own = blocks - stretch + tile * SPAN
    needed = (hits > 0) & (natural[None, None, :] < own[None, :, None])
    before = (index[:, None] < index[None, :]).astype(jnp.bfloat16)
    rank = jnp.einsum("htj,jk->htk", needed.astype(jnp.bfloat16), before, preferred_element_type=jnp.float32)
    rank = jnp.where(needed, rank.astype(jnp.int32) + SPAN, -1)
    spot = jnp.arange(blocks + 2 * GROUP, dtype=jnp.int32)
    hit = rank[:, :, None, :] == spot[None, None, :, None]
    entries = jnp.min(jnp.where(hit, index[None, None, None, :], blocks), axis=3)
    mine = where_is(jnp.minimum(own[:, None] + spot[None, :], blocks - 1))
    entries = jnp.where(spot < SPAN, mine[None], entries)
    steps = (jnp.sum(needed, axis=2, dtype=jnp.int32) + SPAN + GROUP - 1) // GROUP
    return table, entries.astype(jnp.int32), steps.astype(jnp.int32)


def traded(index):
    return index & ~3 | (index & 1) << 1 | (index >> 1) & 1


def seat(index, flip):
    return jnp.where(flip == 1, traded(index), index)


def pack_cache(x, sharers, flip):
    rows, _ = x.shape
    piece_rows = rows // sharers
    some = KV_HEADS // STEPS

    def kernel(flip_ref, in_ref, out_ref):
        for g in range(some):
            for p in range(sharers):
                out_ref[seat(g * sharers + p, flip_ref[0])] = in_ref[p * piece_rows:(p + 1) * piece_rows, g * HEAD_DIM:(g + 1) * HEAD_DIM]

    return pl.pallas_call(
        kernel,
        out_shape=jax.ShapeDtypeStruct((KV_HEADS * sharers, piece_rows, HEAD_DIM), x.dtype),
        grid_spec=pltpu.PrefetchScalarGridSpec(
            num_scalar_prefetch=1,
            grid=(STEPS,),
            in_specs=[pl.BlockSpec((rows, some * HEAD_DIM), lambda i, s: (0, i))],
            out_specs=pl.BlockSpec((some * sharers, piece_rows, HEAD_DIM), lambda i, s: (i, 0, 0)),
        ),
        cost_estimate=pl.CostEstimate(flops=16 * x.size, bytes_accessed=4 * x.size, transcendentals=0),
        name="pack_cache",
    )(flip, x)


def pack_queries(queries, devices, sizes, flip, order):
    rows, width = queries.shape
    heads = sum(sizes)
    some = devices // STEPS

    def kernel(flip_ref, order_ref, q_ref, *out_refs):
        for d in range(some):
            phase = 0
            for size, out_ref in zip(sizes, out_refs):
                for place in range(size):
                    head = order_ref[(pl.program_id(0) * some + d) * heads + phase]
                    at = pl.multiple_of((d * heads + head) * HEAD_DIM, HEAD_DIM)
                    out_ref[seat(d, flip_ref[0]), :, place * HEAD_DIM:(place + 1) * HEAD_DIM] = q_ref[:, pl.ds(at, HEAD_DIM)]
                    phase += 1

    return pl.pallas_call(
        kernel,
        out_shape=[jax.ShapeDtypeStruct((devices, rows, n * HEAD_DIM), queries.dtype) for n in sizes],
        grid_spec=pltpu.PrefetchScalarGridSpec(
            num_scalar_prefetch=2,
            grid=(STEPS,),
            in_specs=[pl.BlockSpec((rows, width // STEPS), lambda i, s, o: (0, i))],
            out_specs=[pl.BlockSpec((some, rows, n * HEAD_DIM), lambda i, s, o: (i, 0, 0)) for n in sizes],
        ),
        cost_estimate=pl.CostEstimate(flops=16 * queries.size, bytes_accessed=4 * queries.size, transcendentals=0),
        name="pack_queries",
    )(flip, order, queries)


def unpack_answers(answers, flip, order):
    devices, rows, _ = answers[0].shape
    sizes = [x.shape[2] // HEAD_DIM for x in answers]
    heads = sum(sizes)
    some = devices // STEPS
    width = devices * heads * HEAD_DIM

    def kernel(flip_ref, order_ref, *refs):
        out_ref = refs[-1]
        for d in range(some):
            phase = 0
            for size, in_ref in zip(sizes, refs):
                for place in range(size):
                    head = order_ref[(pl.program_id(0) * some + d) * heads + phase]
                    at = pl.multiple_of((d * heads + head) * HEAD_DIM, HEAD_DIM)
                    out_ref[:, pl.ds(at, HEAD_DIM)] = in_ref[seat(d, flip_ref[0]), :, place * HEAD_DIM:(place + 1) * HEAD_DIM]
                    phase += 1

    return pl.pallas_call(
        kernel,
        out_shape=jax.ShapeDtypeStruct((rows, width), answers[0].dtype),
        grid_spec=pltpu.PrefetchScalarGridSpec(
            num_scalar_prefetch=2,
            grid=(STEPS,),
            in_specs=[pl.BlockSpec((some, rows, n * HEAD_DIM), lambda i, s, o: (i, 0, 0)) for n in sizes],
            out_specs=pl.BlockSpec((rows, width // STEPS), lambda i, s, o: (0, i)),
        ),
        name="unpack_answers",
    )(flip, order, *answers)


def swapped(x, bit):
    count = lax.axis_size("seq")
    moves = []
    for rep in range(lax.axis_size("rep")):
        turn = traded if rep % 2 else int
        moves += [(rep * count + i, rep * count + turn(turn(i) ^ 1 << bit)) for i in range(count)]
    return lax.ppermute(x, ("rep", "seq"), moves)


def exchanged(x):
    return lax.all_to_all(x, "seq", split_axis=0, concat_axis=0, tiled=True)


def asked_sizes(heads):
    return (1, 1, heads - 2) if heads > 2 else (1,) * heads


def answer_sizes(heads):
    return (heads - 2, 1, 1) if heads > 2 else (1,) * heads


def served_order(vert_count, slash_count, heads, blocks, stretch):
    free = (1 - vert_count / blocks) * (1 - slash_count / (blocks - stretch)) ** SPAN
    free = free.reshape(-1, heads)
    index = jnp.arange(heads, dtype=jnp.int32)
    mine, other = free[:, :, None], free[:, None, :]
    ahead = (other < mine) | ((other == mine) & (index[None, None, :] < index[None, :, None]))
    rank = jnp.sum(ahead, axis=2, dtype=jnp.int32)
    turns = PHASES if heads == len(PHASES) else range(heads)
    ranks = jnp.stack([jnp.sum(jnp.where(rank == r, index, 0), axis=1) for r in turns], axis=1)
    return ranks.astype(jnp.int32)


def body(queries, keys, values, vertical, vert_count, slash, slash_count):
    seq_count = lax.axis_size("seq")
    flip = (lax.axis_index("rep") % 2).astype(jnp.int32).reshape(1)
    position = seat(lax.axis_index("seq"), flip[0])
    query_rows = queries.shape[0]
    key_rows = keys.shape[0]
    sharers = seq_count // KV_HEADS
    heads = QUERY_HEADS // seq_count

    def shared(x):
        pieces = [x]
        for level in range(sharers.bit_length() - 1):
            pieces = pieces + [swapped(y, level) for y in pieces]
        return pieces

    own_keys = exchanged(pack_cache(keys, sharers, flip))
    all_keys = shared(own_keys)
    own_values = exchanged(pack_cache(values, sharers, flip))
    all_values = shared(own_values)
    blocks, stretch = seq_count * key_rows // BLOCK, seq_count * query_rows // BLOCK
    order = served_order(vert_count, slash_count, heads, blocks, stretch)
    mine = position * heads + lax.dynamic_index_in_dim(order, position, 0, keepdims=False)
    order = order.reshape(-1)
    packed = pack_queries(queries, seq_count, asked_sizes(heads), flip, order)
    asked = []
    for size, part in zip(asked_sizes(heads), packed):
        part = exchanged(part).reshape(seq_count * query_rows, -1)
        asked += [(part, h) for h in range(size)]
    piece_blocks = key_rows // sharers // BLOCK
    side = position % sharers
    spot = jnp.arange(seq_count * key_rows // BLOCK, dtype=jnp.int32)
    piece = spot // (seq_count * piece_blocks)
    sender = spot // piece_blocks % seq_count
    natural = (sender * sharers + (piece ^ side)) * piece_blocks + spot % piece_blocks

    def where_is(block):
        piece = block // piece_blocks % sharers ^ side
        return (piece * seq_count + block // (piece_blocks * sharers)) * piece_blocks + block % piece_blocks

    table, entries, steps = make_plan(
        natural, where_is, mine, stretch,
        vertical, vert_count, slash, slash_count,
    )
    plans = [(table[h], entries[h].reshape(-1), steps[h]) for h in range(heads)]
    answers = []
    head = 0
    for size in answer_sizes(heads):
        found = None
        for place in range(size):
            part, h = asked[head]
            found = attention(part, all_keys, all_values, *plans[head], h, place, size, found)
            head += 1
        answers.append(exchanged(found.reshape(seq_count, query_rows, size * HEAD_DIM)))
    return unpack_answers(answers, flip, order)


def solution(mesh):
    return jax.shard_map(
        body,
        mesh=mesh,
        in_specs=(
            P(("rep", "seq"), None),
            P(("rep", "seq"), None),
            P(("rep", "seq"), None),
            P("rep", None),
            P("rep"),
            P("rep", None),
            P("rep"),
        ),
        out_specs=P(("rep", "seq"), None),
        check_vma=False,
    )
```
